32 devices in a mesh: ma: 16 (over z, y, core), row: 2 (over x).
Axes of the slice: x: 2, y: 2, z: 4, core: 2. Of those that a mesh axis runs over, the one named last changes fastest.
Arguments:
- spectral: bfloat16 [384, 2, 384, 2, 769], P('ma', None, 'row'), may hold values from -0.011047363 to 0.011047363
- latitude_basis: bfloat16 [384, 769, 1152], P('ma'), may hold values from -0.21875 to 0.21875
- pair_orders: int32 [384], replicated, may hold values from 0 to 383, each once
Outputs:
- grid_values: bfloat16 [64, 2, 1152, 2304], P('row', None, 'ma')
The draws below stay inside these ranges and needn't reach their ends.
Inputs may be any that keep to these rules, and one draw needn't show every extreme that they name: A permutation of 0 to 383; slot p holds the orders pair_orders[p] and 767 - pair_orders[p].
All inputs are finite; a program needn't handle non-finite values.
Results may differ from the reference program's by a relative error of at most 0.0066.
Values may be sent and summed in bfloat16 or wider, within the bound.
A program may use at most 192 MiB of HBM per device.

```python
import math
import jax
import jax.numpy as jnp
from jax import lax

L = 768
NCHEB = 384
NLAT = 1152
NLON = 2304
FIELDS = 2
LEV = 64
PAIRS = 384
PACKED = 769


def shard_levels(stream_key, dims, shards, smallest, largest):
    def one(axis_at, blocks):
        heights = jax.random.uniform(jax.random.fold_in(jax.random.fold_in(stream_key, 6), axis_at), (blocks,), jnp.float32, smallest / len(shards), largest / len(shards))
        return jnp.repeat(jnp.exp(heights), dims[axis_at] // blocks).reshape((-1,) + (1,) * (len(dims) - axis_at - 1))

    gain = one(*shards[0])
    for cut in shards[1:]:
        gain = gain * one(*cut)
    return gain


def normal_values(rng, extent, width, reach, cuts=(), held_as=jnp.bfloat16):
    factor_of = shard_levels(rng, extent, cuts, -0.22, 0.18) if cuts else 1.0
    array = jax.random.normal(rng, extent, jnp.float32) * width * factor_of
    return jnp.minimum(jnp.maximum(array, -reach), reach).astype(held_as)


def setup_inputs(seed: int = 0) -> dict:
    key_list = jax.random.split(jax.random.key(seed), 4)
    spectral = normal_values(key_list[0], (PAIRS, 2, NCHEB, FIELDS, PACKED), (1.0 / (NCHEB * L) ** 0.5), 0.011047363, ((0, 16), (2, 2)))
    latitude_basis = normal_values(key_list[1], (PAIRS, PACKED, NLAT), PACKED ** -0.5, 0.21875, ((0, 16),))
    pair_orders = jax.random.permutation(key_list[2], PAIRS).astype(jnp.int32)
    return dict(spectral=spectral, latitude_basis=latitude_basis, pair_orders=pair_orders)


def radial_table(total_modes, levels):
    mode_index = lax.broadcasted_iota(jnp.int32, (total_modes, levels), 0)
    points = lax.broadcasted_iota(jnp.int32, (total_modes, levels), 1)
    period = 2 * (total_modes - 1)
    phase_steps = (mode_index * points) % period
    return jnp.cos(phase_steps.astype(jnp.float32) * (2.0 * math.pi / period)).astype(jnp.bfloat16)


def longitude_table(pair_orders, degrees, points):
    lower_orders = pair_orders.astype(jnp.int32)
    orders = jnp.stack([lower_orders, degrees - 1 - lower_orders], axis=1)
    weights = jnp.where(orders == 0, 1.0, 2.0).astype(jnp.float32)
    phase_index = (orders[:, :, None] * lax.broadcasted_iota(jnp.int32, (1, 1, points), 2)) % points
    angles = phase_index.astype(jnp.float32) * (2.0 * math.pi / points)
    real_part = weights[:, :, None] * jnp.cos(angles)
    imag_part = -weights[:, :, None] * jnp.sin(angles)
    stacked = jnp.stack([real_part, imag_part], axis=2)
    return stacked.reshape(-1, points).astype(jnp.bfloat16)


def reference(spectral, latitude_basis, pair_orders):
    cheb_table = radial_table(NCHEB, LEV).astype(jnp.float32)
    lon_table = longitude_table(pair_orders, L, NLON).astype(jnp.float32)
    packed_rows = jnp.arange(PACKED, dtype=jnp.int32)

    def one_pair(pair_index):
        coeffs = lax.dynamic_index_in_dim(spectral, pair_index, 0, keepdims=False)
        basis_rows = lax.dynamic_index_in_dim(latitude_basis, pair_index, 0, keepdims=False)
        lower_order = lax.dynamic_index_in_dim(pair_orders, pair_index, 0, keepdims=False).astype(jnp.int32)
        below_split = packed_rows < (L - lower_order)
        selectors = jnp.stack([below_split, jnp.logical_not(below_split)], axis=0).astype(jnp.float32)
        summed = jnp.einsum("ckfr,kl->lfcr", coeffs.astype(jnp.float32), cheb_table)
        levels = lax.optimization_barrier(summed.astype(jnp.bfloat16)).astype(jnp.float32)
        masked = levels[None] * selectors[:, None, None, None, :]
        fourier = jnp.einsum("hlfcr,rt->lfhct", masked, basis_rows.astype(jnp.float32))
        return fourier.astype(jnp.bfloat16)

    fourier_all = lax.map(one_pair, jnp.arange(PAIRS, dtype=jnp.int32))
    stacked = jnp.transpose(fourier_all, (1, 2, 5, 0, 3, 4)).reshape(LEV, FIELDS, NLAT, PAIRS * 4)

    def one_level(level_block):
        return jnp.einsum("fto,on->ftn", level_block.astype(jnp.float32), lon_table).astype(jnp.bfloat16)

    return lax.map(one_level, stacked)
```

```python
import functools
import math

import jax
import jax.numpy as jnp
from jax import lax
from jax.experimental import pallas as pl
from jax.experimental.pallas import tpu as pltpu
from jax.sharding import PartitionSpec as P

NLON = 2304
LEV = 64
CHUNKS = 2
TILE = 24


def radial_table(total_modes, levels):
    mode_index = lax.broadcasted_iota(jnp.int32, (total_modes, levels), 0)
    points = lax.broadcasted_iota(jnp.int32, (total_modes, levels), 1)
    period = 2 * (total_modes - 1)
    phase_steps = mode_index * points % period
    return jnp.cos(phase_steps.astype(jnp.float32) * (2.0 * math.pi / period)).astype(jnp.bfloat16)


def longitude_table(pair_orders, degrees, points):
    orders = jnp.stack([pair_orders, degrees - 1 - pair_orders], axis=0)
    weights = jnp.where(orders == 0, 1.0, 2.0).astype(jnp.float32)
    phase_index = orders[:, :, None] * lax.broadcasted_iota(jnp.int32, (1, 1, points), 2) % points
    angles = phase_index.astype(jnp.float32) * (2.0 * math.pi / points)
    real_part = weights[:, :, None] * jnp.cos(angles)
    imag_part = -weights[:, :, None] * jnp.sin(angles)
    stacked = jnp.stack([real_part.astype(jnp.bfloat16), imag_part.astype(jnp.bfloat16)], axis=1)
    return stacked.reshape(-1, points)


def order_selectors(local_orders, degrees, packed):
    packed_rows = lax.broadcasted_iota(jnp.int32, (local_orders.shape[0], packed), 1)
    below_split = packed_rows < (degrees - local_orders)[:, None]
    return jnp.stack([below_split, jnp.logical_not(below_split)], axis=1).astype(jnp.bfloat16)


def synth_kernel(subs, tile, *refs):
    count = piece_count(subs)
    pieces, table_ref, out_ref, rows_ref = refs[:count], refs[count], refs[-2], refs[-1]
    images = out_ref.shape[0]
    points = out_ref.shape[2]

    def gather(t, carry):
        slot = 0
        for piece, start, size in subs:
            block = pieces[piece][:, t]
            block = block[:, start : start + size].astype(jnp.float32)
            turned = block.reshape(-1, block.shape[-1]).T
            for part in range(turned.shape[0] // images):
                for lane in range(turned.shape[1] // 128):
                    rows_ref[slot, pl.ds(t, images, stride=tile), :] = turned[
                        part * images : (part + 1) * images, lane * 128 : (lane + 1) * 128
                    ]
                    slot += 1
        return carry

    lax.fori_loop(0, tile, gather, 0)
    rows = jnp.concatenate(
        [rows_ref[slot].astype(jnp.bfloat16) for slot in range(rows_ref.shape[0])], axis=1
    )
    width = points // 3
    for cut in range(3):
        cols = slice(cut * width, (cut + 1) * width)
        sums = jnp.dot(rows, table_ref[:, cols], preferred_element_type=jnp.float32)
        out_ref[:, :, cols] = sums.reshape(images, tile, width).astype(jnp.bfloat16)


def piece_count(subs):
    return 1 + max(piece for piece, _, _ in subs)


def synthesize(pieces, subs, table, whole, images, chunk, total):
    lats, lanes = pieces[0].shape[1], pieces[0].shape[3]
    points = table.shape[1]
    tile = TILE
    in_specs = [
        pl.BlockSpec((p.shape[0], tile, p.shape[2], lanes), lambda t: (0, t, 0, 0)) for p in pieces
    ]
    in_specs.append(pl.BlockSpec(table.shape, lambda t: (0, 0)))
    operands = list(pieces) + [table]
    aliases = {}
    if whole is not None:
        in_specs.append(pl.BlockSpec(memory_space=pl.ANY))
        aliases = {len(operands): 0}
        operands.append(whole)
    return pl.pallas_call(
        functools.partial(synth_kernel, tuple(subs), tile),
        grid=(lats // tile,),
        in_specs=in_specs,
        out_specs=pl.BlockSpec((images, tile, points), lambda t: (chunk, t, 0)),
        out_shape=jax.ShapeDtypeStruct((total, lats, points), jnp.bfloat16),
        scratch_shapes=[pltpu.VMEM((table.shape[0] // 128, images * tile, 128), jnp.float32)],
        input_output_aliases=aliases,
        compiler_params=pltpu.CompilerParams(vmem_limit_bytes=60 * 1024 * 1024),
        cost_estimate=pl.CostEstimate(
            flops=2 * images * lats * points * table.shape[0],
            bytes_accessed=2 * (images * lats * (points + table.shape[0]) + table.size),
            transcendentals=0,
        ),
        name="synthesize",
    )(*operands)


def per_device(spectral, latitude_basis, pair_orders):
    pair_dev, parts, local_modes, fields, packed = spectral.shape
    degrees = packed - 1
    row_count = lax.axis_size("row")
    ma_count = lax.axis_size("ma")
    lats = latitude_basis.shape[2]
    own_lats = lats // ma_count
    row = lax.axis_index("row")
    total_modes = local_modes * row_count
    level_dev = LEV // row_count
    step = level_dev // CHUNKS
    lanes = 2 * parts * step * fields
    fused = own_lats % TILE == 0 and pair_dev % 8 == 0 and lanes == 128 and ma_count % 16 == 0
    if fused and pair_dev > 8:
        splits = [[(0, 8), (8, pair_dev)]] + [[(0, pair_dev)]] * (CHUNKS - 1)
        groups = [(0, 8), (8, pair_dev)]
    else:
        splits = [[(0, pair_dev)]] * CHUNKS
        groups = [(0, pair_dev)]
    cheb_table = radial_table(total_modes, LEV)
    own_rows = lax.dynamic_slice_in_dim(cheb_table, row * local_modes, local_modes, 0)
    local_orders = lax.dynamic_slice_in_dim(
        pair_orders, lax.axis_index("ma") * pair_dev, pair_dev, 0
    )
    selectors = order_selectors(local_orders, degrees, packed)
    by_owner = pair_orders.reshape(ma_count, pair_dev)
    lon_table = jnp.concatenate(
        [longitude_table(by_owner[:, a:b].reshape(-1), degrees, NLON) for a, b in groups], axis=0
    )

    def partial(owner, chunk):
        table = lax.dynamic_slice_in_dim(own_rows, owner * level_dev + chunk * step, step, 1)
        return jnp.einsum("pckfr,kl->pclfr", spectral, table, preferred_element_type=jnp.float32)

    def received(chunk):
        hops = []
        for hop in range(1, row_count):
            away = partial((row + hop) % row_count, chunk).astype(jnp.bfloat16)
            ring = [(i, (i + hop) % row_count) for i in range(row_count)]
            parts_of = []
            for a, b in splits[chunk]:
                parts_of.append(lax.ppermute(away[a:b], "row", ring))
            hops.append(parts_of)
        return hops

    whole, outs = None, []
    for chunk in range(CHUNKS):
        hops = received(chunk)
        own = partial(row, chunk)
        pieces = []
        for part, (a, b) in enumerate(splits[chunk]):
            total = own[a:b]
            for hop in hops:
                total = total + hop[part].astype(jnp.float32)
            levels = total.astype(jnp.bfloat16)
            own_selectors, levels = lax.optimization_barrier((selectors[a:b], levels))
            masked = levels[:, None] * own_selectors[:, :, None, None, None, :]
            masked = masked.reshape(b - a, lanes, packed)
            fourier = jnp.einsum(
                "prt,pmr->tpm", latitude_basis[a:b], masked, preferred_element_type=jnp.float32
            ).astype(jnp.bfloat16)
            got = lax.all_to_all(fourier, "ma", split_axis=0, concat_axis=0, tiled=True)
            pieces.append(got.reshape(ma_count, own_lats, b - a, lanes))
        if fused:
            if len(pieces) > 1:
                subs = [(n, 0, b - a) for n, (a, b) in enumerate(groups)]
            else:
                subs = [(0, a, b - a) for a, b in groups]
            whole = synthesize(
                pieces, subs, lon_table, whole, step * fields, chunk, level_dev * fields
            )
        else:
            got = pieces[0].reshape(ma_count, own_lats, pair_dev, 2 * parts, step * fields)
            got = jnp.transpose(got, (4, 1, 3, 0, 2)).reshape(step * fields, own_lats, -1)
            synthesized = jnp.einsum(
                "ito,on->itn", got, lon_table, preferred_element_type=jnp.float32
            ).astype(jnp.bfloat16)
            outs.append(synthesized)
    if not fused:
        whole = jnp.concatenate(outs, axis=0)
    return whole.reshape(level_dev, fields, own_lats, NLON)


def solution(mesh):
    return jax.shard_map(
        per_device,
        mesh=mesh,
        in_specs=(P("ma", None, "row", None, None), P("ma", None, None), P()),
        out_specs=P("row", None, "ma", None),
        check_vma=False,
    )
```
